32 devices in a mesh: row: 8 (over y, x, core), col: 4 (over z).
Axes of the slice: x: 2, y: 2, z: 4, core: 2. Of those that a mesh axis runs over, the one named last changes fastest.
Arguments:
- covariance: bfloat16 [16384, 16384], P('row', 'col'), may hold values from -0.12 to 0.6, as said below
- estimate: bfloat16 [16384, 16384], P('row', 'col'), may hold values from -2.3 to 12, as said below
- dual_var: bfloat16 [16384, 16384], P('row', 'col'), may hold values from -1.7 to 1.7, as said below
- start_basis: float32 [16384, 128], P('row'), may hold values from -6 to 6
Outputs:
- next_estimate: float32 [16384, 16384], P('row', 'col')
- next_dual: bfloat16 [16384, 16384], P('row', 'col')
The draws below stay inside these ranges and needn't reach their ends.
Inputs may be any that keep to these rules, and one draw needn't show every extreme that they name: `covariance`: symmetric. `estimate`: symmetric. `dual_var`: symmetric.
All inputs are finite; a program needn't handle non-finite values.
Results may differ from the reference program's by a relative error of at most 0.001.
Values sent between devices are 32-bit elements; how exact they have to be, the bound alone decides.
A program may use at most 192 MiB of HBM per device.

```python
import jax
import jax.numpy as jnp
from jax import lax

P_SIZE = 16384
RANK = 128
ITERS = 1
NS_ITERS = 12
N_ROW = 8


def symmetric_part(key, spread):
    raw_draw = jax.random.truncated_normal(key, -4.0, 4.0, (P_SIZE, P_SIZE), jnp.float32)
    return (raw_draw + raw_draw.T) * (spread * 0.7071067811865476)


def on_diagonal():
    row_ids = lax.broadcasted_iota(jnp.int32, (P_SIZE, 1), 0)
    col_ids = lax.broadcasted_iota(jnp.int32, (1, P_SIZE), 1)
    return row_ids == col_ids


def draw_covariance(key, part):
    off_diag = symmetric_part(jax.random.fold_in(key, 11), 0.005)
    variances = jax.random.uniform(jax.random.fold_in(key, 12), (P_SIZE,), jnp.float32, 0.05, 0.15)
    matrix = jnp.where(on_diagonal(), variances[:, None], off_diag)
    return matrix.astype(jnp.bfloat16)


def draw_estimate(key, part):
    off_diag = symmetric_part(jax.random.fold_in(key, 21), 0.4)
    diagonal = jax.random.uniform(jax.random.fold_in(key, 22), (P_SIZE,), jnp.float32, 8.0, 12.0)
    return jnp.where(on_diagonal(), diagonal[:, None], off_diag).astype(jnp.bfloat16)


def draw_dual_var(key, part):
    return symmetric_part(jax.random.fold_in(key, 31), 0.3).astype(jnp.bfloat16)


def steps_of(stream_key, shape, split, least, top_value):
    def one(dim, blocks):
        steps = jax.random.uniform(jax.random.fold_in(jax.random.fold_in(stream_key, 6), dim), (blocks,), jnp.float32, least / len(split), top_value / len(split))
        return jnp.repeat(jnp.exp(steps), shape[dim] // blocks).reshape((-1,) + (1,) * (len(shape) - dim - 1))

    gain = one(*split[0])
    for cut in split[1:]:
        gain = gain * one(*cut)
    return gain


def bell_draw(stream_key, extent, scale, limit, cuts=(), kind=jnp.bfloat16):
    array = scale * jax.random.normal(stream_key, extent, jnp.float32)
    if cuts:
        array = array * steps_of(stream_key, extent, cuts, -0.22, 0.18)
    return jnp.clip(array, -limit, limit).astype(kind)


def setup_inputs(seed: int = 0) -> dict:
    keys = jax.random.split(jax.random.key(seed), 5)
    return {
        "covariance": draw_covariance(jax.random.fold_in(keys[4], 71), 0),
        "estimate": draw_estimate(jax.random.fold_in(keys[4], 71), 0),
        "dual_var": draw_dual_var(jax.random.fold_in(keys[4], 71), 0),
        "start_basis": bell_draw(keys[3], (P_SIZE, RANK), 1.0, 6.0, ((0, 8),), jnp.float32),
    }


penalty = 0.01
threshold = 0.2
base_level = 10.0
highest = lax.Precision.HIGHEST

def inner_product(left_side, right_side):
    return lax.dot_general(left_side.astype(jnp.float32), right_side.astype(jnp.float32), (((0,), (0,)), ((), ())), precision=highest, preferred_element_type=jnp.float32)

def normalize(mapped, gram_matrix):
    lower_factor = jnp.linalg.cholesky(gram_matrix)
    identity = jnp.eye(gram_matrix.shape[0], dtype=jnp.float32)
    inverse = lax.linalg.triangular_solve(lower_factor, identity, left_side=True, lower=True)
    return jnp.dot(mapped.astype(jnp.float32), inverse.T.astype(jnp.float32), precision=highest, preferred_element_type=jnp.float32)

def response_of(ritz_matrix):
    identity = jnp.eye(ritz_matrix.shape[0], dtype=jnp.float32)
    square = jnp.dot(ritz_matrix.astype(jnp.float32), ritz_matrix.astype(jnp.float32), precision=highest, preferred_element_type=jnp.float32) + 4.0 * penalty * identity
    frobenius = jnp.sqrt(jnp.sum(square * square))

    def newton(sweep_index, state_pair):
        iterate, partner = state_pair
        factor = 0.5 * (3.0 * identity - jnp.dot(partner.astype(jnp.float32), iterate.astype(jnp.float32), precision=highest, preferred_element_type=jnp.float32))
        return (jnp.dot(iterate.astype(jnp.float32), factor.astype(jnp.float32), precision=highest, preferred_element_type=jnp.float32), jnp.dot(factor.astype(jnp.float32), partner.astype(jnp.float32), precision=highest, preferred_element_type=jnp.float32))
    iterate, partner = lax.fori_loop(0, NS_ITERS, newton, (square / frobenius, identity))
    square_root = jnp.sqrt(frobenius) * iterate
    return (ritz_matrix + square_root) / (2.0 * penalty) - base_level * identity

def reference(covariance, estimate, dual_var, start_basis):
    shifted = penalty * (estimate.astype(jnp.float32) - dual_var.astype(jnp.float32)) - covariance.astype(jnp.float32)
    current = start_basis
    for sweep_index in range(ITERS):
        mapped = jnp.dot(shifted.astype(jnp.float32), current.astype(jnp.float32), precision=highest, preferred_element_type=jnp.float32)
        current = normalize(mapped, inner_product(mapped, mapped))
    product = jnp.dot(shifted.astype(jnp.float32), current.astype(jnp.float32), precision=highest, preferred_element_type=jnp.float32)
    raw_ritz = inner_product(current, product)
    ritz_matrix = 0.5 * (raw_ritz + raw_ritz.T)
    response = response_of(ritz_matrix)
    weighted = jnp.dot(current.astype(jnp.float32), response.astype(jnp.float32), precision=highest, preferred_element_type=jnp.float32)
    rows_block = P_SIZE // N_ROW

    def finish(block_index):
        row_start = block_index * rows_block
        left_rows = lax.dynamic_slice_in_dim(weighted, row_start, rows_block, 0)
        theta_tile = lax.dot_general(left_rows.astype(jnp.float32), current.astype(jnp.float32), (((1,), (1,)), ((), ())), precision=highest, preferred_element_type=jnp.float32)
        row_ids = row_start + lax.broadcasted_iota(jnp.int32, (rows_block, 1), 0)
        col_ids = lax.broadcasted_iota(jnp.int32, (1, P_SIZE), 1)
        theta_tile = theta_tile + jnp.where(row_ids == col_ids, base_level, 0.0)
        dual_rows = lax.dynamic_slice_in_dim(dual_var, row_start, rows_block, 0)
        mixture = theta_tile + dual_rows.astype(jnp.float32)
        clipped = jnp.clip(mixture, -threshold, threshold)
        return (mixture - clipped, clipped.astype(jnp.bfloat16))
    new_estimate, new_dual = lax.map(finish, jnp.arange(N_ROW, dtype=jnp.int32))
    return (new_estimate.reshape(P_SIZE, P_SIZE), new_dual.reshape(P_SIZE, P_SIZE))
```

```python
import functools

import jax
import jax.numpy as jnp
from jax import lax
from jax.experimental import pallas as pl
from jax.experimental.pallas import tpu as pltpu
from jax.sharding import PartitionSpec as P

NS_ITERS = 12


penalty = 0.01
threshold = 0.2
base_level = 10.0
highest = lax.Precision.HIGHEST


def from_root(value, axis, source):
    kept = jnp.where(lax.axis_index(axis) == source, value, 0).astype(value.dtype)
    return lax.psum(kept, axis)


def inner_product(left_side, right_side):
    return lax.dot_general(
        left_side,
        right_side,
        (((0,), (0,)), ((), ())),
        precision=highest,
        preferred_element_type=jnp.float32,
    )


def normalize(mapped, gram_matrix):
    lower_factor = jnp.linalg.cholesky(gram_matrix)
    identity = jnp.eye(gram_matrix.shape[0], dtype=jnp.float32)
    inverse = lax.linalg.triangular_solve(lower_factor, identity, left_side=True, lower=True)
    return jnp.dot(mapped, inverse.T, precision=highest, preferred_element_type=jnp.float32)


def response_of(ritz_matrix):
    identity = jnp.eye(ritz_matrix.shape[0], dtype=jnp.float32)
    square = (
        jnp.dot(ritz_matrix, ritz_matrix, precision=highest, preferred_element_type=jnp.float32)
        + 4.0 * penalty * identity
    )
    frobenius = jnp.sqrt(jnp.sum(square * square))

    def newton(sweep_index, state_pair):
        iterate, partner = state_pair
        factor = 0.5 * (
            3.0 * identity
            - jnp.dot(partner, iterate, precision=highest, preferred_element_type=jnp.float32)
        )
        return (
            jnp.dot(iterate, factor, precision=highest, preferred_element_type=jnp.float32),
            jnp.dot(factor, partner, precision=highest, preferred_element_type=jnp.float32),
        )

    iterate, partner = lax.fori_loop(0, NS_ITERS, newton, (square / frobenius, identity))
    square_root = jnp.sqrt(frobenius) * iterate
    return (ritz_matrix + square_root) / (2.0 * penalty) - base_level * identity


def column_basis(shifted, row_basis):
    partial_terms = lax.dot_general(
        shifted,
        row_basis,
        (((0,), (0,)), ((), ())),
        precision=highest,
        preferred_element_type=jnp.float32,
    )
    mapped = lax.psum(partial_terms, "row")
    gram_matrix = lax.psum(inner_product(mapped, mapped), "col")
    return normalize(mapped, gram_matrix)


def row_image(shifted, col_basis):
    local_terms = jnp.dot(shifted, col_basis, precision=highest, preferred_element_type=jnp.float32)
    return lax.psum(local_terms, "col")


def row_inner(left_side, right_side):
    return lax.psum(inner_product(left_side, right_side), "row")


def plain_body(covariance, estimate, dual_var, start_basis):
    shifted = penalty * (
        estimate.astype(jnp.float32) - dual_var.astype(jnp.float32)
    ) - covariance.astype(jnp.float32)
    rows_tile = shifted.shape[0]
    cols_tile = shifted.shape[1]
    row_basis = start_basis
    col_basis = column_basis(shifted, row_basis)
    blocks_per_column = lax.axis_size("row") // lax.axis_size("col")
    row_index = lax.axis_index("row")
    own_block = lax.dynamic_slice_in_dim(
        col_basis, row_index % blocks_per_column * rows_tile, rows_tile, 0
    )
    row_basis = from_root(own_block, "col", row_index // blocks_per_column)
    product = row_image(shifted, col_basis)
    raw_ritz = row_inner(row_basis, product)
    ritz_matrix = 0.5 * (raw_ritz + raw_ritz.T)
    response = response_of(ritz_matrix)
    weighted = jnp.dot(row_basis, response, precision=highest, preferred_element_type=jnp.float32)
    theta_tile = lax.dot_general(
        weighted,
        col_basis,
        (((1,), (1,)), ((), ())),
        precision=highest,
        preferred_element_type=jnp.float32,
    )
    row_ids = row_index * rows_tile + lax.broadcasted_iota(jnp.int32, (rows_tile, 1), 0)
    col_ids = lax.axis_index("col") * cols_tile + lax.broadcasted_iota(jnp.int32, (1, cols_tile), 1)
    theta_tile = theta_tile + jnp.where(row_ids == col_ids, base_level, 0.0)
    mixture = theta_tile + dual_var.astype(jnp.float32)
    clipped = jnp.clip(mixture, -threshold, threshold)
    return (mixture - clipped, clipped.astype(jnp.bfloat16))


MESH = pl.DeviceIdType.MESH
VMEM = pl.BlockSpec(memory_space=pltpu.VMEM)
VMEM_BYTES = 60 * 1024 * 1024
FULL_VMEM = 67043328
LOADS_AHEAD = 3


def high_dot(left_side, right_side, dims):
    return lax.dot_general(
        left_side, right_side, (dims, ((), ())), precision=highest, preferred_element_type=jnp.float32
    )


def split(value):
    upper = value.astype(jnp.bfloat16)
    return upper, (value - upper.astype(jnp.float32)).astype(jnp.bfloat16)


def flip(value, mask, size):
    result, bit = 0, 1
    while bit < size:
        result += (value // bit + mask // bit) % 2 * bit
        bit *= 2
    return result


def front_kernel(
    n_row, n_col, est_hbm, dual_hbm, cov_hbm, basis_hbm, mc_ref, mr_ref, out_ref,
    tiles, basis_ref, left_ref, image_ref, away, near, other, zbuf, load_sems, basis_sem, *sems
):
    send1, recv1, send2, recv2, send3, recv3, send4, recv4, send5, recv5, send6, recv6 = sems
    row, col = lax.axis_index("row"), lax.axis_index("col")
    rank, piece = mc_ref.shape[1:]
    rows_tile = tiles.shape[2]
    chips = n_row // 2
    chip, core = row // 2, row % 2
    sibling = chip * 2 + 1 - core
    ratio = n_row // n_col
    group = n_row // ratio
    matrices = (est_hbm, dual_hbm, cov_hbm)

    def load(which, step):
        there = flip(chip, chips - 1 - step // 2, chips)
        where = 2 * there + (1 - core + step) % 2
        columns = pl.ds(pl.multiple_of(where * piece, piece), piece)
        return pltpu.make_async_copy(
            matrices[which].at[:, columns], tiles.at[which, where], load_sems.at[which, step]
        )

    start_basis = pltpu.make_async_copy(basis_hbm, basis_ref, basis_sem)
    start_basis.start()
    for step in range(LOADS_AHEAD):
        for which in range(3):
            load(which, step).start()

    barrier = pltpu.get_barrier_semaphore()

    def greet_row(t, carry):
        pl.semaphore_signal(barrier, inc=1, device_id=((row + t) % n_row, col), device_id_type=MESH)
        return carry

    def greet_col(t, carry):
        pl.semaphore_signal(barrier, inc=1, device_id=(row, (col + t) % n_col), device_id_type=MESH)
        return carry

    lax.fori_loop(1, n_row, greet_row, 0)
    lax.fori_loop(1, n_col, greet_col, 0)

    start_basis.wait()
    depth = min(256, rows_tile)
    for index in range(rows_tile // depth):
        where = slice(index * depth, (index + 1) * depth)
        upper, lower = split(basis_ref[where, :].T)
        left_ref[:rank, where] = upper
        left_ref[rank:, where] = lower
    pl.semaphore_wait(barrier, n_row - 1 + n_col - 1)

    def copy(src, dst, send, recv, target):
        return pltpu.make_async_remote_copy(
            src_ref=src, dst_ref=dst, send_sem=send, recv_sem=recv, device_id=target, device_id_type=MESH
        )

    def image_part(step):
        @pl.when(step + LOADS_AHEAD < n_row)
        def _():
            for which in range(3):
                load(which, step + LOADS_AHEAD).start()

        for which in range(3):
            load(which, step).wait()
        where = 2 * flip(chip, chips - 1 - step // 2, chips) + (1 - core + step) % 2

        def product(which):
            return jnp.dot(left_ref[...], tiles[which, where], preferred_element_type=jnp.float32)

        both = penalty * (product(0) - product(1)) - product(2)
        return both[:rank] + both[rank:]

    def to_sibling(t):
        return copy(away.at[t], near.at[t], send1.at[t], recv1.at[t], (sibling, col))

    def to_chip(t):
        there = flip(chip, chips - 1 - t, chips)
        return copy(near.at[t], other.at[t], send2.at[t], recv2.at[t], (2 * there + core, col))

    def sweep(t, carry):
        away[t] = image_part(2 * t)
        to_sibling(t).start()
        part = image_part(2 * t + 1)
        to_sibling(t).wait_recv()
        near[t] = near[t] + part

        @pl.when(t < chips - 1)
        def _():
            to_chip(t).start()

        return carry

    lax.fori_loop(0, chips, sweep, 0)
    total = near[chips - 1]
    for t in range(chips - 1):
        to_chip(t).wait_recv()
        total += other[t]
    mc_ref[row] = total

    own = mc_ref.at[row]

    def along(source, way):
        block = own if source is None else zbuf.at[source]
        source = col if source is None else source
        return copy(
            block, zbuf.at[source], send4.at[(way + 1) // 2, source], recv4.at[source], (row, col + way)
        )

    @pl.when(col + 1 < n_col)
    def _():
        along(None, 1).start()

    @pl.when(col >= 1)
    def _():
        along(None, -1).start()

    def plane(t):
        return copy(own, own, send3.at[t], recv3.at[t], (2 * flip(chip, t + 1, chips) + core, col))

    def arrived(t):
        return mc_ref.at[2 * flip(chip, t, chips) + core]

    def pair(t):
        block = arrived(t)
        return copy(block, block, send5.at[t], recv5.at[t], (sibling, col))

    for t in range(chips - 1):
        plane(t).start()
    pair(0).start()

    def onward(source):
        target = source * ratio + row // group
        slot = row % group
        return copy(zbuf.at[source], mr_ref.at[slot], send6.at[source], recv6.at[slot], (target, col)), target

    def serve(source, way):
        @pl.when((source >= 0) & (source < n_col))
        def _():
            along(source, way).wait_recv()

            @pl.when((col + way >= 0) & (col + way < n_col))
            def _():
                along(source, way).start()

            hop, target = onward(source)

            @pl.when(target != row)
            def _():
                hop.start()

            @pl.when(target == row)
            def _():
                mr_ref[row % group] = zbuf[source]

    def serve_both(s):
        serve(col - s, 1)
        serve(col + s, -1)

    image_ref[...] = jnp.zeros_like(image_ref)
    strip = min(512, rows_tile)

    def apply(where):
        upper, lower = split(mc_ref[where].T)
        right = jnp.concatenate([upper, lower], axis=1)

        def one(index, carry):
            rows = pl.ds(pl.multiple_of(index * strip, strip), strip)

            def product(which):
                return jnp.dot(tiles[which, where, rows, :], right, preferred_element_type=jnp.float32)

            image_ref[rows, :] += penalty * (product(0) - product(1)) - product(2)
            return carry

        lax.fori_loop(0, rows_tile // strip, one, 0)

    def apply_chip(t, swap):
        apply(2 * flip(chip, t, chips) + (core + swap) % 2)

    def wait_pair(t):
        block = mc_ref.at[2 * flip(chip, t, chips) + 1 - core]
        copy(own, block, send5.at[t], recv5.at[t], (sibling, col)).wait_recv()

    def take(t):
        copy(own, arrived(t), send3.at[t - 1], recv3.at[t - 1], (row, col)).wait_recv()
        pair(t).start()

    apply_chip(0, 0)
    out_ref[:rank] = high_dot(own[...], own[...], ((1,), (1,)))
    wait_pair(0)
    apply_chip(0, 1)
    served = 1
    for t in range(1, chips - 1):
        take(t)
    serve_both(served)
    served += 1

    def middle(t, carry):
        apply_chip(t, 0)
        wait_pair(t)
        apply_chip(t, 1)
        return carry

    lax.fori_loop(1, chips - 1, middle, 0)
    take(chips - 1)
    if served < n_col:
        serve_both(served)
        served += 1
    lax.fori_loop(chips - 1, chips, middle, 0)
    for s in range(served, n_col):
        serve_both(s)

    @pl.when(row // ratio == col)
    def _():
        for k in range(group):
            mr_ref[k] = mc_ref[(row % ratio) * group + k]

    ritz = jnp.zeros((rank, rank), jnp.float32)
    for k in range(group):
        @pl.when((row // ratio != col) & ((row % ratio) * group + k != row))
        def _():
            copy(zbuf.at[0], mr_ref.at[k], send6.at[0], recv6.at[k], (sibling, col)).wait_recv()

        rows = slice(k * piece, (k + 1) * piece)
        ritz += high_dot(
            mr_ref[k], image_ref[rows, :rank] + image_ref[rows, rank:], ((1,), (0,))
        )
    out_ref[rank:] = ritz

    for t in range(chips):
        to_sibling(t).wait_send()
        pair(t).wait_send()
    for t in range(chips - 1):
        to_chip(t).wait_send()
        plane(t).wait_send()

    @pl.when(col + 1 < n_col)
    def _():
        along(None, 1).wait_send()

    @pl.when(col >= 1)
    def _():
        along(None, -1).wait_send()

    for s in range(1, n_col):
        for source, way in ((col - s, 1), (col + s, -1)):
            @pl.when((source >= 0) & (source < n_col))
            def _():
                @pl.when((col + way >= 0) & (col + way < n_col))
                def _():
                    along(source, way).wait_send()

                hop, target = onward(source)

                @pl.when(target != row)
                def _():
                    hop.wait_send()


def front(matrices, start_basis, n_row, n_col):
    rows_tile, cols_tile = matrices[0].shape
    rank = start_basis.shape[1]
    piece = cols_tile // n_row
    chips, ratio = n_row // 2, n_row // n_col
    group = n_row // ratio
    dma = pltpu.SemaphoreType.DMA
    return pl.pallas_call(
        functools.partial(front_kernel, n_row, n_col),
        in_specs=[pl.BlockSpec(memory_space=pl.ANY)] * 4,
        out_specs=(VMEM, VMEM, VMEM),
        out_shape=(
            jax.ShapeDtypeStruct((n_row, rank, piece), jnp.float32),
            jax.ShapeDtypeStruct((group, rank, piece), jnp.float32),
            jax.ShapeDtypeStruct((2 * rank, rank), jnp.float32),
        ),
        scratch_shapes=[
            pltpu.VMEM((3, n_row, rows_tile, piece), jnp.bfloat16),
            pltpu.VMEM((rows_tile, rank), jnp.float32),
            pltpu.VMEM((2 * rank, rows_tile), jnp.bfloat16),
            pltpu.VMEM((rows_tile, 2 * rank), jnp.float32),
            pltpu.VMEM((chips, rank, piece), jnp.float32),
            pltpu.VMEM((chips, rank, piece), jnp.float32),
            pltpu.VMEM((chips - 1, rank, piece), jnp.float32),
            pltpu.VMEM((n_col, rank, piece), jnp.float32),
            dma((3, n_row)), dma,
            dma((chips,)), dma((chips,)),
            dma((chips - 1,)), dma((chips - 1,)),
            dma((chips - 1,)), dma((chips - 1,)),
            dma((2, n_col)), dma((n_col,)),
            dma((chips,)), dma((chips,)),
            dma((n_col,)), dma((group,)),
        ],
        compiler_params=pltpu.CompilerParams(
            collective_id=0, has_side_effects=True, vmem_limit_bytes=FULL_VMEM
        ),
    )(*matrices, start_basis)


def total_kernel(n_row, n_col, term_ref, out_ref, terms, part, planes, *sems):
    send1, recv1, send2, recv2, send3, recv3 = sems
    row, col = lax.axis_index("row"), lax.axis_index("col")
    barrier = pltpu.get_barrier_semaphore()

    def greet_row(t, carry):
        pl.semaphore_signal(barrier, inc=1, device_id=((row + t) % n_row, col), device_id_type=MESH)
        return carry

    def greet_col(t, carry):
        pl.semaphore_signal(barrier, inc=1, device_id=(row, (col + t) % n_col), device_id_type=MESH)
        return carry

    lax.fori_loop(1, n_row, greet_row, 0)
    lax.fori_loop(1, n_col, greet_col, 0)
    pl.semaphore_wait(barrier, n_row - 1 + n_col - 1)

    def copy(src, dst, send, recv, target):
        return pltpu.make_async_remote_copy(
            src_ref=src, dst_ref=dst, send_sem=send, recv_sem=recv, device_id=target, device_id_type=MESH
        )

    first = []
    for t in range(1, n_row):
        there = (row + t) % n_row
        first.append(copy(term_ref.at[there], terms.at[t], send1.at[t], recv1.at[t], (there, col)))
        first[-1].start()
    summed = term_ref[row]
    for t in range(1, n_row):
        first[t - 1].wait_recv()
        summed += terms[t]
    part[...] = summed
    second = []
    for t in range(1, n_col):
        there = (col + t) % n_col
        second.append(copy(part, planes.at[col], send2.at[t], recv2.at[col], (row, there)))
        second[-1].start()
    planes[col] = summed
    for t in range(1, n_col):
        source = (col + t) % n_col
        copy(part, planes.at[source], send2.at[t], recv2.at[source], (row, source)).wait_recv()
    out_ref[row] = jnp.sum(planes[...], axis=0)
    third = []
    for t in range(1, n_row):
        there = (row + t) % n_row
        third.append(copy(out_ref.at[row], out_ref.at[row], send3.at[t], recv3.at[t], (there, col)))
        third[-1].start()
    for t in range(1, n_row):
        source = (row + n_row - t) % n_row
        copy(out_ref.at[row], out_ref.at[source], send3.at[t], recv3.at[t], (source, col)).wait_recv()
    for item in first + second + third:
        item.wait_send()


def total(terms, n_row, n_col):
    blocks = terms.reshape(n_row, terms.shape[0] // n_row, terms.shape[1])
    block = blocks.shape[1:]
    dma = pltpu.SemaphoreType.DMA
    summed = pl.pallas_call(
        functools.partial(total_kernel, n_row, n_col),
        in_specs=[VMEM],
        out_specs=VMEM,
        out_shape=jax.ShapeDtypeStruct(blocks.shape, jnp.float32),
        scratch_shapes=[
            pltpu.VMEM(blocks.shape, jnp.float32),
            pltpu.VMEM(block, jnp.float32),
            pltpu.VMEM((n_col, *block), jnp.float32),
            dma((n_row,)), dma((n_row,)),
            dma((n_col,)), dma((n_col,)),
            dma((n_row,)), dma((n_row,)),
        ],
        compiler_params=pltpu.CompilerParams(collective_id=1, has_side_effects=True),
    )(blocks)
    return summed.reshape(terms.shape)


def weight_kernel(moment_ref, rows_ref, out_ref, inverse_ref, ritz_ref, iterate_ref, partner_ref):
    rank = rows_ref.shape[1]
    row_ids = lax.broadcasted_iota(jnp.int32, (rank, rank), 0)
    col_ids = lax.broadcasted_iota(jnp.int32, (rank, rank), 1)
    line_ids = lax.broadcasted_iota(jnp.int32, (1, rank), 1)
    identity = jnp.where(row_ids == col_ids, 1.0, 0.0)
    inverse = moment_ref[:rank]
    for k in range(rank):
        pivot = 1.0 / inverse[k : k + 1, k : k + 1]
        column = inverse[:, k : k + 1]
        line = jnp.where(line_ids == k, 1.0, inverse[k : k + 1, :]) * pivot
        inverse = jnp.where(
            row_ids == k, line, jnp.where(col_ids == k, 0.0, inverse) - column * line
        )
    inverse_ref[...] = inverse
    raw = moment_ref[rank:]
    iterate_ref[...] = 0.5 * (raw + raw.T)
    plain = ((1,), (0,))
    ritz_ref[...] = high_dot(inverse_ref[...], iterate_ref[...], plain)
    square = high_dot(ritz_ref[...], ritz_ref[...], plain) + 4.0 * penalty * identity
    frobenius = jnp.sqrt(jnp.sum(square * square.T, keepdims=True))
    iterate_ref[...] = square / frobenius
    partner_ref[...] = identity

    def newton(step, carry):
        iterate, partner = iterate_ref[...], partner_ref[...]
        factor = 0.5 * (3.0 * identity - high_dot(partner, iterate, plain))
        iterate_ref[...] = high_dot(iterate, factor, plain)
        partner_ref[...] = high_dot(factor, partner, plain)
        return carry

    lax.fori_loop(0, NS_ITERS, newton, 0)
    root = jnp.sqrt(frobenius) * iterate_ref[...]
    response = (ritz_ref[...] + root) / (2.0 * penalty) - base_level * identity
    partner_ref[...] = high_dot(response, inverse_ref[...], plain)
    piece = rows_ref.shape[2]
    for k in range(rows_ref.shape[0]):
        out_ref[k * piece : (k + 1) * piece, :] = high_dot(rows_ref[k].T, partner_ref[...], plain)


def finish_kernel(weighted_ref, cols_ref, dual_ref, est_ref, clip_ref, right_ref, low_ref):
    step = pl.program_id(0)
    count, rank, piece = cols_ref.shape
    depth = dual_ref.shape[0]

    @pl.when(step == 0)
    def _():
        for k in range(count):
            upper, lower = split(cols_ref[k])
            right_ref[k, :rank] = upper
            right_ref[k, rank:] = upper
            low_ref[k] = lower

    upper, lower = split(weighted_ref[...])
    both = jnp.concatenate([upper, lower], axis=1)
    n_grid = pl.num_programs(0)
    row_start = (lax.axis_index("row") * n_grid + step) * depth
    gap = (
        lax.broadcasted_iota(jnp.int32, (depth, piece), 1)
        - lax.broadcasted_iota(jnp.int32, (depth, piece), 0)
    )
    for k in range(count):
        where = slice(k * piece, (k + 1) * piece)
        col_start = lax.axis_index("col") * (count * piece) + k * piece
        theta = jnp.dot(both, right_ref[k], preferred_element_type=jnp.float32)
        theta += jnp.dot(upper, low_ref[k], preferred_element_type=jnp.float32)
        theta += jnp.where(gap == row_start - col_start, base_level, 0.0)
        mixture = theta + dual_ref[:, where].astype(jnp.float32)
        clipped = jnp.clip(mixture, -threshold, threshold)
        est_ref[:, where] = mixture - clipped
        clip_ref[:, where] = clipped.astype(jnp.bfloat16)


def finish(weighted, cols, dual_var):
    rows_tile, cols_tile = dual_var.shape
    count, rank, piece = cols.shape
    depth = min(512, rows_tile)
    wide = pl.BlockSpec((depth, cols_tile), lambda step: (step, 0))
    return pl.pallas_call(
        finish_kernel,
        grid=(rows_tile // depth,),
        in_specs=[
            pl.BlockSpec((depth, rank), lambda step: (step, 0)),
            pl.BlockSpec(cols.shape, lambda step: (0, 0, 0)),
            wide,
        ],
        out_specs=(wide, wide),
        out_shape=(
            jax.ShapeDtypeStruct(dual_var.shape, jnp.float32),
            jax.ShapeDtypeStruct(dual_var.shape, jnp.bfloat16),
        ),
        scratch_shapes=[
            pltpu.VMEM((count, 2 * rank, piece), jnp.bfloat16),
            pltpu.VMEM((count, rank, piece), jnp.bfloat16),
        ],
        compiler_params=pltpu.CompilerParams(
            dimension_semantics=("arbitrary",), vmem_limit_bytes=VMEM_BYTES
        ),
    )(weighted, cols, dual_var)


def fast_body(n_row, n_col, covariance, estimate, dual_var, start_basis):
    rows_tile, cols_tile = covariance.shape
    rank = start_basis.shape[1]
    matrices = (estimate, dual_var, covariance)
    cols, rows, moments = front(matrices, start_basis, n_row, n_col)
    moments = total(moments, n_row, n_col)
    weighted = pl.pallas_call(
        weight_kernel,
        in_specs=[VMEM, VMEM],
        out_specs=VMEM,
        out_shape=jax.ShapeDtypeStruct((rows_tile, rank), jnp.float32),
        scratch_shapes=[pltpu.VMEM((rank, rank), jnp.float32)] * 4,
        compiler_params=pltpu.CompilerParams(vmem_limit_bytes=VMEM_BYTES),
    )(moments, rows)
    return finish(weighted, cols, dual_var)


def body(covariance, estimate, dual_var, start_basis):
    n_row, n_col = lax.axis_size("row"), lax.axis_size("col")
    rows_tile, cols_tile = covariance.shape
    rank = start_basis.shape[1]
    piece = cols_tile // n_row
    fits = (
        n_row % 2 == 0
        and n_row % n_col == 0
        and cols_tile % n_row == 0
        and piece % 128 == 0
        and rows_tile % piece == 0
        and rank % 128 == 0
        and 2 * rank % (8 * n_row) == 0
        and n_row & (n_row - 1) == 0
        and n_row > LOADS_AHEAD
        and 6 * rows_tile * cols_tile + 18 * rank * cols_tile <= FULL_VMEM
    )
    if not fits:
        return plain_body(covariance, estimate, dual_var, start_basis)
    return fast_body(n_row, n_col, covariance, estimate, dual_var, start_basis)


def solution(mesh):
    return jax.shard_map(
        body,
        mesh=mesh,
        in_specs=(P("row", "col"), P("row", "col"), P("row", "col"), P("row", None)),
        out_specs=(P("row", "col"), P("row", "col")),
        check_vma=False,
    )
```

```python
import functools

import jax
import jax.numpy as jnp
from jax import lax
from jax.experimental import pallas as pl
from jax.experimental.pallas import tpu as pltpu
from jax.sharding import PartitionSpec as P

NS_ITERS = 12


penalty = 0.01
threshold = 0.2
base_level = 10.0
highest = lax.Precision.HIGHEST


def from_root(value, axis, source):
    kept = jnp.where(lax.axis_index(axis) == source, value, 0).astype(value.dtype)
    return lax.psum(kept, axis)


def inner_product(left_side, right_side):
    return lax.dot_general(
        left_side,
        right_side,
        (((0,), (0,)), ((), ())),
        precision=highest,
        preferred_element_type=jnp.float32,
    )


def normalize(mapped, gram_matrix):
    lower_factor = jnp.linalg.cholesky(gram_matrix)
    identity = jnp.eye(gram_matrix.shape[0], dtype=jnp.float32)
    inverse = lax.linalg.triangular_solve(lower_factor, identity, left_side=True, lower=True)
    return jnp.dot(mapped, inverse.T, precision=highest, preferred_element_type=jnp.float32)


def response_of(ritz_matrix):
    identity = jnp.eye(ritz_matrix.shape[0], dtype=jnp.float32)
    square = (
        jnp.dot(ritz_matrix, ritz_matrix, precision=highest, preferred_element_type=jnp.float32)
        + 4.0 * penalty * identity
    )
    frobenius = jnp.sqrt(jnp.sum(square * square))

    def newton(sweep_index, state_pair):
        iterate, partner = state_pair
        factor = 0.5 * (
            3.0 * identity
            - jnp.dot(partner, iterate, precision=highest, preferred_element_type=jnp.float32)
        )
        return (
            jnp.dot(iterate, factor, precision=highest, preferred_element_type=jnp.float32),
            jnp.dot(factor, partner, precision=highest, preferred_element_type=jnp.float32),
        )

    iterate, partner = lax.fori_loop(0, NS_ITERS, newton, (square / frobenius, identity))
    square_root = jnp.sqrt(frobenius) * iterate
    return (ritz_matrix + square_root) / (2.0 * penalty) - base_level * identity


def column_basis(shifted, row_basis):
    partial_terms = lax.dot_general(
        shifted,
        row_basis,
        (((0,), (0,)), ((), ())),
        precision=highest,
        preferred_element_type=jnp.float32,
    )
    mapped = lax.psum(partial_terms, "row")
    gram_matrix = lax.psum(inner_product(mapped, mapped), "col")
    return normalize(mapped, gram_matrix)


def row_image(shifted, col_basis):
    local_terms = jnp.dot(shifted, col_basis, precision=highest, preferred_element_type=jnp.float32)
    return lax.psum(local_terms, "col")


def row_inner(left_side, right_side):
    return lax.psum(inner_product(left_side, right_side), "row")


def plain_body(covariance, estimate, dual_var, start_basis):
    shifted = penalty * (
        estimate.astype(jnp.float32) - dual_var.astype(jnp.float32)
    ) - covariance.astype(jnp.float32)
    rows_tile = shifted.shape[0]
    cols_tile = shifted.shape[1]
    row_basis = start_basis
    col_basis = column_basis(shifted, row_basis)
    blocks_per_column = lax.axis_size("row") // lax.axis_size("col")
    row_index = lax.axis_index("row")
    own_block = lax.dynamic_slice_in_dim(
        col_basis, row_index % blocks_per_column * rows_tile, rows_tile, 0
    )
    row_basis = from_root(own_block, "col", row_index // blocks_per_column)
    product = row_image(shifted, col_basis)
    raw_ritz = row_inner(row_basis, product)
    ritz_matrix = 0.5 * (raw_ritz + raw_ritz.T)
    response = response_of(ritz_matrix)
    weighted = jnp.dot(row_basis, response, precision=highest, preferred_element_type=jnp.float32)
    theta_tile = lax.dot_general(
        weighted,
        col_basis,
        (((1,), (1,)), ((), ())),
        precision=highest,
        preferred_element_type=jnp.float32,
    )
    row_ids = row_index * rows_tile + lax.broadcasted_iota(jnp.int32, (rows_tile, 1), 0)
    col_ids = lax.axis_index("col") * cols_tile + lax.broadcasted_iota(jnp.int32, (1, cols_tile), 1)
    theta_tile = theta_tile + jnp.where(row_ids == col_ids, base_level, 0.0)
    mixture = theta_tile + dual_var.astype(jnp.float32)
    clipped = jnp.clip(mixture, -threshold, threshold)
    return (mixture - clipped, clipped.astype(jnp.bfloat16))


MESH = pl.DeviceIdType.MESH
VMEM = pl.BlockSpec(memory_space=pltpu.VMEM)
VMEM_BYTES = 60 * 1024 * 1024
FULL_VMEM = 67043328
LOADS_AHEAD = 3
CHUNKS = 4
FINISH_ROWS = 512


def high_dot(left_side, right_side, dims):
    return lax.dot_general(
        left_side, right_side, (dims, ((), ())), precision=highest, preferred_element_type=jnp.float32
    )


def split(value):
    upper = value.astype(jnp.bfloat16)
    return upper, (value - upper.astype(jnp.float32)).astype(jnp.bfloat16)


def remote(src, dst, send, recv, target):
    return pltpu.make_async_remote_copy(
        src_ref=src, dst_ref=dst, send_sem=send, recv_sem=recv, device_id=target, device_id_type=MESH
    )


def flip(value, mask, size):
    result, bit = 0, 1
    while bit < size:
        result += (value // bit + mask // bit) % 2 * bit
        bit *= 2
    return result


def front_kernel(
    n_row, n_col, est_hbm, dual_hbm, cov_hbm, basis_hbm, weights_hbm, right_hbm, low_hbm,
    tiles, basis_ref, left_ref, image_ref, away, near, other, zbuf, mc_ref, mr_ref,
    gram, gram_terms, gram_part, gram_planes, gram_sum,
    inner, inner_terms, inner_part, inner_planes, inner_sum,
    inverse_ref, ritz_ref, iterate_ref, partner_ref,
    load_sems, basis_sem, store_sems, *sems
):
    send1, recv1, send2, recv2, send3, recv3, send4, recv4, send5, recv5, send6, recv6 = sems[:12]
    gram_scatter, gram_across, gram_gather, gram_finish, gram_drain = sum_over_mesh(
        n_row, n_col, gram, gram_terms, gram_part, gram_planes, gram_sum, sems[12:18]
    )
    inner_scatter, inner_across, inner_gather, inner_finish, inner_drain = sum_over_mesh(
        n_row, n_col, inner, inner_terms, inner_part, inner_planes, inner_sum, sems[18:24]
    )
    copy = remote
    row, col = lax.axis_index("row"), lax.axis_index("col")
    rank, piece = mc_ref.shape[1:]
    rows_tile = tiles.shape[2]
    chips = n_row // 2
    chip, core = row // 2, row % 2
    sibling = chip * 2 + 1 - core
    ratio = n_row // n_col
    group = n_row // ratio
    cut = rank // CHUNKS
    home = row // ratio

    def works(left, right):
        odd = (left + right) % 2
        return (left == right) | ((odd == 1) & (left < right)) | ((odd == 0) & (left > right))

    working = works(home, col)
    matrices = (est_hbm, dual_hbm, cov_hbm)

    def load(which, step):
        there = flip(chip, chips - 1 - step // 2, chips)
        where = 2 * there + (1 - core + step) % 2
        columns = pl.ds(pl.multiple_of(where * piece, piece), piece)
        return pltpu.make_async_copy(
            matrices[which].at[:, columns], tiles.at[which, where], load_sems.at[which, step]
        )

    start_basis = pltpu.make_async_copy(basis_hbm, basis_ref, basis_sem)
    start_basis.start()
    for step in range(LOADS_AHEAD):
        for which in range(3):
            load(which, step).start()

    barrier = pltpu.get_barrier_semaphore()

    def greet_row(t, carry):
        pl.semaphore_signal(barrier, inc=1, device_id=((row + t) % n_row, col), device_id_type=MESH)
        return carry

    def greet_col(t, carry):
        pl.semaphore_signal(barrier, inc=1, device_id=(row, (col + t) % n_col), device_id_type=MESH)
        return carry

    lax.fori_loop(1, n_row, greet_row, 0)
    lax.fori_loop(1, n_col, greet_col, 0)

    start_basis.wait()
    depth = min(256, rows_tile)
    for index in range(rows_tile // depth):
        where = slice(index * depth, (index + 1) * depth)
        upper, lower = split(basis_ref[where, :].T)
        left_ref[:rank, where] = upper
        left_ref[rank:, where] = lower
    pl.semaphore_wait(barrier, n_row - 1 + n_col - 1)

    def image_part(step):
        @pl.when(step + LOADS_AHEAD < n_row)
        def _():
            for which in range(3):
                load(which, step + LOADS_AHEAD).start()

        for which in range(3):
            load(which, step).wait()
        where = 2 * flip(chip, chips - 1 - step // 2, chips) + (1 - core + step) % 2

        def product(which):
            return jnp.dot(left_ref[...], tiles[which, where], preferred_element_type=jnp.float32)

        both = penalty * (product(0) - product(1)) - product(2)
        return both[:rank] + both[rank:]

    def to_sibling(t):
        return copy(away.at[t], near.at[t], send1.at[t], recv1.at[t], (sibling, col))

    def to_chip(t):
        there = flip(chip, chips - 1 - t, chips)
        return copy(near.at[t], other.at[t], send2.at[t], recv2.at[t], (2 * there + core, col))

    def sweep(t, carry):
        away[t] = image_part(2 * t)
        to_sibling(t).start()
        part = image_part(2 * t + 1)
        to_sibling(t).wait_recv()
        near[t] = near[t] + part

        @pl.when(t < chips - 1)
        def _():
            to_chip(t).start()

        return carry

    lax.fori_loop(0, chips, sweep, 0)
    total = near[chips - 1]
    for t in range(chips - 1):
        to_chip(t).wait_recv()
        total += other[t]
    mc_ref[row] = total

    own = mc_ref.at[row]

    def along(source, way, part):
        block = own if source is None else zbuf.at[source]
        source = col if source is None else source
        lines = pl.ds(part * cut, cut)
        return copy(
            block.at[lines], zbuf.at[source, lines],
            send4.at[(way + 1) // 2, source, part], recv4.at[source, part], (row, col + way),
        )

    def start_along(parts):
        for part in parts:
            @pl.when(col + 1 < n_col)
            def _():
                along(None, 1, part).start()

            @pl.when(col >= 1)
            def _():
                along(None, -1, part).start()

    wide = double(own[...], 0)
    wide = lax.dot_general(
        wide, wide, (((1,), (1,)), ((), ())), preferred_element_type=jnp.float32
    )
    wide = wide[:rank] + wide[rank:]
    gram[...] = (wide[:, :rank] + wide[:, rank:]).reshape(gram.shape)
    gram_scatter()
    start_along(range(CHUNKS // 2))

    def plane(t):
        return copy(own, own, send3.at[t], recv3.at[t], (2 * flip(chip, t + 1, chips) + core, col))

    def arrived(t):
        return mc_ref.at[2 * flip(chip, t, chips) + core]

    def pair(t):
        block = arrived(t)
        return copy(block, block, send5.at[t], recv5.at[t], (sibling, col))

    for t in range(chips - 2):
        plane(t).start()
    pair(0).start()

    def onward(source, part):
        target = source * ratio + row // group
        slot = row % group
        lines = pl.ds(part * cut, cut)
        hop = copy(
            zbuf.at[source, lines], mr_ref.at[slot, lines],
            send6.at[source, part], recv6.at[slot, part], (target, col),
        )
        return hop, target

    def send_onward(source, part):
        hop, target = onward(source, part)

        @pl.when(target != row)
        def _():
            hop.start()

        @pl.when(target == row)
        def _():
            lines = slice(part * cut, (part + 1) * cut)
            mr_ref[row % group, lines] = zbuf[source, lines]

    def serve(source, way, part):
        @pl.when((source >= 0) & (source < n_col))
        def _():
            along(source, way, part).wait_recv()

            @pl.when((col + way >= 0) & (col + way < n_col))
            def _():
                along(source, way, part).start()

            @pl.when(works(source, col))
            def _():
                send_onward(source, part)

    def serve_half(hop, half):
        for part in range(CHUNKS // 2):
            for k in range(2):
                @pl.when(half == k)
                def _():
                    serve(col - hop, 1, k * (CHUNKS // 2) + part)
                    serve(col + hop, -1, k * (CHUNKS // 2) + part)

    image_ref[...] = jnp.zeros_like(image_ref)
    strip = min(512, rows_tile)

    def apply(where):
        upper, lower = split(mc_ref[where].T)
        right = jnp.concatenate([upper, lower], axis=1)

        def one(index, carry):
            rows = pl.ds(pl.multiple_of(index * strip, strip), strip)

            def product(which):
                return jnp.dot(tiles[which, where, rows, :], right, preferred_element_type=jnp.float32)

            image_ref[rows, :] += penalty * (product(0) - product(1)) - product(2)
            return carry

        lax.fori_loop(0, rows_tile // strip, one, 0)

    def apply_chip(t, swap):
        apply(2 * flip(chip, t, chips) + (core + swap) % 2)

    def wait_pair(t):
        block = mc_ref.at[2 * flip(chip, t, chips) + 1 - core]
        copy(own, block, send5.at[t], recv5.at[t], (sibling, col)).wait_recv()

    def take(t):
        copy(own, arrived(t), send3.at[t - 1], recv3.at[t - 1], (row, col)).wait_recv()
        pair(t).start()

    def stage(j, carry):
        t = j // 2

        @pl.when(j == 2)
        def _():
            gram_gather()
            plane(chips - 2).start()
            for other_chip in range(1, chips - 1):
                take(other_chip)

        @pl.when(j == n_row - 3)
        def _():
            take(chips - 1)

        @pl.when(j % 2 == 1)
        def _():
            wait_pair(t)

        @pl.when(working)
        def _():
            apply_chip(t, j % 2)

        @pl.when(j == 0)
        def _():
            gram_across()
            start_along(range(CHUNKS // 2, CHUNKS))

        @pl.when(t + 1 < n_col)
        def _():
            serve_half(t + 1, j % 2)

        @pl.when(j == 2 * n_col - 3)
        def _():
            for source in range(n_col):
                @pl.when((source != col) & jnp.logical_not(works(source, col)))
                def _():
                    for part in range(CHUNKS):
                        send_onward(source, part)

        return carry

    lax.fori_loop(0, n_row, stage, 0)
    gram_finish()
    third = -(-rank // 24) * 8
    inverse_ref[...] = gram_sum[...].reshape(rank, rank)

    def wait_rows():
        for k in range(group):
            @pl.when((home != col) & ((row % ratio) * group + k != row))
            def _():
                for part in range(CHUNKS):
                    lines = pl.ds(part * cut, cut)
                    copy(
                        zbuf.at[0, lines], mr_ref.at[k, lines],
                        send6.at[0, part], recv6.at[k, part], (sibling, col),
                    ).wait_recv()

    @pl.when(home == col)
    def _():
        for k in range(group):
            mr_ref[k] = mc_ref[(row % ratio) * group + k]

    @pl.when(working)
    def _():
        wait_rows()
        ritz = jnp.zeros((2 * rank, 2 * rank), jnp.float32)
        for k in range(group):
            rows = slice(k * piece, (k + 1) * piece)
            ritz += jnp.dot(
                double(mr_ref[k], 0),
                double(image_ref[rows, :rank] + image_ref[rows, rank:], 1),
                preferred_element_type=jnp.float32,
            )
        ritz = ritz[:rank] + ritz[rank:]
        times = jnp.where(home == col, 1.0, 2.0)
        inner[...] = (times * (ritz[:, :rank] + ritz[:, rank:])).reshape(inner.shape)

    @pl.when(jnp.logical_not(working))
    def _():
        inner[...] = jnp.zeros_like(inner)

    inner_scatter()
    inverse_ref[...] = invert(inverse_ref[...], 0, third)
    inner_across()
    inverse_ref[...] = invert(inverse_ref[...], third, 2 * third)
    inner_gather()
    inverse_ref[...] = invert(inverse_ref[...], 2 * third, rank)

    def prepare(k, carry):
        upper, lower = split(mc_ref[k])
        tiles[0, k, :rank, :] = upper
        tiles[0, k, rank : 2 * rank, :] = upper
        tiles[1, k, :rank, :] = lower
        return carry

    lax.fori_loop(0, n_row, prepare, 0)
    store_right = pltpu.make_async_copy(
        tiles.at[0, :, pl.ds(0, 2 * rank)], right_hbm, store_sems.at[0]
    )
    store_low = pltpu.make_async_copy(tiles.at[1, :, pl.ds(0, rank)], low_hbm, store_sems.at[1])
    store_right.start()
    store_low.start()
    inner_finish()
    update = response_times_inverse(
        inner_sum[...].reshape(rank, rank), inverse_ref, ritz_ref, iterate_ref, partner_ref
    )
    partner_ref[...] = update

    @pl.when(jnp.logical_not(working))
    def _():
        wait_rows()

    for k in range(group):
        tiles[2, 0, k * piece : (k + 1) * piece, : 2 * rank] = double(
            fine_dot(mr_ref[k].T, partner_ref[...]), 1
        )
    store_weights = pltpu.make_async_copy(
        tiles.at[2, 0, :, pl.ds(0, 2 * rank)], weights_hbm, store_sems.at[2]
    )
    store_weights.start()
    gram_drain()
    inner_drain()
    for t in range(chips):
        to_sibling(t).wait_send()
        pair(t).wait_send()
    for t in range(chips - 1):
        to_chip(t).wait_send()
        plane(t).wait_send()

    for part in range(CHUNKS):
        @pl.when(col + 1 < n_col)
        def _():
            along(None, 1, part).wait_send()

        @pl.when(col >= 1)
        def _():
            along(None, -1, part).wait_send()

        for s in range(1, n_col):
            for source, way in ((col - s, 1), (col + s, -1)):
                @pl.when((source >= 0) & (source < n_col))
                def _():
                    @pl.when((col + way >= 0) & (col + way < n_col))
                    def _():
                        along(source, way, part).wait_send()

                    hop, target = onward(source, part)

                    @pl.when(target != row)
                    def _():
                        hop.wait_send()

    store_right.wait()
    store_low.wait()
    store_weights.wait()


def front(matrices, start_basis, n_row, n_col):
    rows_tile, cols_tile = matrices[0].shape
    rank = start_basis.shape[1]
    piece = cols_tile // n_row
    chips, ratio = n_row // 2, n_row // n_col
    group = n_row // ratio
    dma = pltpu.SemaphoreType.DMA
    block = (rank // n_row, rank)
    sum_buffers = [
        pltpu.VMEM((n_row, *block), jnp.float32),
        pltpu.VMEM((n_row, *block), jnp.float32),
        pltpu.VMEM(block, jnp.float32),
        pltpu.VMEM((n_col, *block), jnp.float32),
        pltpu.VMEM((n_row, *block), jnp.float32),
    ]
    sum_sems = [dma((n_row,))] * 2 + [dma((n_col,))] * 2 + [dma((n_row,))] * 2
    return pl.pallas_call(
        functools.partial(front_kernel, n_row, n_col),
        in_specs=[pl.BlockSpec(memory_space=pl.ANY)] * 4,
        out_specs=[pl.BlockSpec(memory_space=pl.ANY)] * 3,
        out_shape=(
            jax.ShapeDtypeStruct((rows_tile, 2 * rank), jnp.bfloat16),
            jax.ShapeDtypeStruct((n_row, 2 * rank, piece), jnp.bfloat16),
            jax.ShapeDtypeStruct((n_row, rank, piece), jnp.bfloat16),
        ),
        scratch_shapes=[
            pltpu.VMEM((3, n_row, rows_tile, piece), jnp.bfloat16),
            pltpu.VMEM((rows_tile, rank), jnp.float32),
            pltpu.VMEM((2 * rank, rows_tile), jnp.bfloat16),
            pltpu.VMEM((rows_tile, 2 * rank), jnp.float32),
            pltpu.VMEM((chips, rank, piece), jnp.float32),
            pltpu.VMEM((chips, rank, piece), jnp.float32),
            pltpu.VMEM((chips - 1, rank, piece), jnp.float32),
            pltpu.VMEM((n_col, rank, piece), jnp.float32),
            pltpu.VMEM((n_row, rank, piece), jnp.float32),
            pltpu.VMEM((group, rank, piece), jnp.float32),
            *sum_buffers, *sum_buffers,
            *[pltpu.VMEM((rank, rank), jnp.float32)] * 4,
            dma((3, n_row)), dma, dma((3,)),
            dma((chips,)), dma((chips,)),
            dma((chips - 1,)), dma((chips - 1,)),
            dma((chips - 1,)), dma((chips - 1,)),
            dma((2, n_col, CHUNKS)), dma((n_col, CHUNKS)),
            dma((chips,)), dma((chips,)),
            dma((n_col, CHUNKS)), dma((group, CHUNKS)),
            *sum_sems, *sum_sems,
        ],
        compiler_params=pltpu.CompilerParams(
            collective_id=0, has_side_effects=True, vmem_limit_bytes=FULL_VMEM
        ),
    )(*matrices, start_basis)


def sum_over_mesh(n_row, n_col, term, terms, part, planes, out, sems):
    send1, recv1, send2, recv2, send3, recv3 = sems
    row, col = lax.axis_index("row"), lax.axis_index("col")

    def first(t):
        there = (row + t) % n_row
        return remote(term.at[there], terms.at[t], send1.at[t], recv1.at[t], (there, col))

    def second(t):
        there = (col + t) % n_col
        return remote(part, planes.at[col], send2.at[t], recv2.at[col], (row, there))

    def third(t):
        there = (row + t) % n_row
        return remote(out.at[row], out.at[row], send3.at[t], recv3.at[t], (there, col))

    def scatter():
        for t in range(1, n_row):
            first(t).start()

    def across():
        summed = term[row]
        for t in range(1, n_row):
            first(t).wait_recv()
            summed += terms[t]
        part[...] = summed
        for t in range(1, n_col):
            second(t).start()
        planes[col] = summed

    def gather():
        for t in range(1, n_col):
            source = (col + t) % n_col
            remote(part, planes.at[source], send2.at[t], recv2.at[source], (row, source)).wait_recv()
        out[row] = jnp.sum(planes[...], axis=0)
        for t in range(1, n_row):
            third(t).start()

    def finish():
        for t in range(1, n_row):
            source = (row + n_row - t) % n_row
            remote(out.at[row], out.at[source], send3.at[t], recv3.at[t], (source, col)).wait_recv()

    def drain():
        for t in range(1, n_row):
            first(t).wait_send()
            third(t).wait_send()
        for t in range(1, n_col):
            second(t).wait_send()

    return scatter, across, gather, finish, drain


def invert(value, first, last):
    rank = value.shape[0]
    row_ids = lax.broadcasted_iota(jnp.int32, (rank, rank), 0)
    col_ids = lax.broadcasted_iota(jnp.int32, (rank, rank), 1)
    line_ids = lax.broadcasted_iota(jnp.int32, (1, rank), 1)
    for k in range(first, last):
        pivot = 1.0 / value[k : k + 1, k : k + 1]
        column = value[:, k : k + 1]
        line = jnp.where(line_ids == k, 1.0, value[k : k + 1, :]) * pivot
        value = jnp.where(
            row_ids == k, line, jnp.where(col_ids == k, 0.0, value) - column * line
        )
    return value


def double(value, axis):
    return jnp.concatenate(split(value), axis=axis)


def fine_dot(left_side, right_side):
    right = double(right_side, 1)
    both = jnp.dot(
        double(left_side, 1),
        jnp.concatenate([right, right], axis=0),
        preferred_element_type=jnp.float32,
    )
    width = right_side.shape[1]
    return both[:, :width] + both[:, width:]


def response_times_inverse(raw, inverse_ref, ritz_ref, iterate_ref, partner_ref):
    rank = raw.shape[0]
    row_ids = lax.broadcasted_iota(jnp.int32, (rank, rank), 0)
    col_ids = lax.broadcasted_iota(jnp.int32, (rank, rank), 1)
    identity = jnp.where(row_ids == col_ids, 1.0, 0.0)
    ritz_ref[...] = fine_dot(inverse_ref[...], 0.5 * (raw + raw.T))
    square = fine_dot(ritz_ref[...], ritz_ref[...]) + 4.0 * penalty * identity
    frobenius = jnp.sqrt(jnp.sum(square * square.T, keepdims=True))
    start = square / frobenius
    factor = 1.5 * identity - 0.5 * start
    iterate_ref[...] = fine_dot(start, factor)
    partner_ref[...] = factor

    def newton(step, carry):
        iterate, partner = iterate_ref[...], partner_ref[...]
        factor = 1.5 * identity - 0.5 * fine_dot(partner, iterate)
        iterate_ref[...] = fine_dot(iterate, factor)
        partner_ref[...] = fine_dot(factor, partner)
        return carry

    lax.fori_loop(1, NS_ITERS, newton, 0)
    root = jnp.sqrt(frobenius) * iterate_ref[...]
    response = (ritz_ref[...] + root) / (2.0 * penalty) - base_level * identity
    return fine_dot(response, inverse_ref[...])


def finish_kernel(weights_ref, right_ref, low_ref, dual_ref, est_ref, clip_ref):
    step = pl.program_id(0)
    count, rank, piece = low_ref.shape
    depth = dual_ref.shape[0]
    n_grid = pl.num_programs(0)
    row_start = (lax.axis_index("row") * n_grid + step) * depth
    gap = (
        lax.broadcasted_iota(jnp.int32, (depth, piece), 1)
        - lax.broadcasted_iota(jnp.int32, (depth, piece), 0)
    )
    for k in range(count):
        where = slice(k * piece, (k + 1) * piece)
        col_start = lax.axis_index("col") * (count * piece) + k * piece
        theta = jnp.dot(weights_ref[...], right_ref[k], preferred_element_type=jnp.float32)
        theta += jnp.dot(weights_ref[:, :rank], low_ref[k], preferred_element_type=jnp.float32)
        theta += jnp.where(gap == row_start - col_start, base_level, 0.0)
        mixture = theta + dual_ref[:, where].astype(jnp.float32)
        clipped = jnp.clip(mixture, -threshold, threshold)
        est_ref[:, where] = mixture - clipped
        clip_ref[:, where] = clipped.astype(jnp.bfloat16)


def finish(weights, right, low, dual_var):
    rows_tile, cols_tile = dual_var.shape
    depth = min(FINISH_ROWS, rows_tile)
    wide = pl.BlockSpec((depth, cols_tile), lambda step: (step, 0))
    return pl.pallas_call(
        finish_kernel,
        grid=(rows_tile // depth,),
        in_specs=[
            pl.BlockSpec((depth, weights.shape[1]), lambda step: (step, 0)),
            pl.BlockSpec(right.shape, lambda step: (0, 0, 0)),
            pl.BlockSpec(low.shape, lambda step: (0, 0, 0)),
            wide,
        ],
        out_specs=(wide, wide),
        out_shape=(
            jax.ShapeDtypeStruct(dual_var.shape, jnp.float32),
            jax.ShapeDtypeStruct(dual_var.shape, jnp.bfloat16),
        ),
        compiler_params=pltpu.CompilerParams(
            dimension_semantics=("arbitrary",), vmem_limit_bytes=VMEM_BYTES
        ),
    )(weights, right, low, dual_var)


def fast_body(n_row, n_col, covariance, estimate, dual_var, start_basis):
    rows_tile, cols_tile = covariance.shape
    rank = start_basis.shape[1]
    matrices = (estimate, dual_var, covariance)
    weights, right, low = front(matrices, start_basis, n_row, n_col)
    return finish(weights, right, low, dual_var)


def body(covariance, estimate, dual_var, start_basis):
    n_row, n_col = lax.axis_size("row"), lax.axis_size("col")
    rows_tile, cols_tile = covariance.shape
    rank = start_basis.shape[1]
    piece = cols_tile // n_row
    fits = (
        n_row % 2 == 0
        and n_row % n_col == 0
        and cols_tile % n_row == 0
        and piece % 128 == 0
        and rows_tile % piece == 0
        and rank % 128 == 0
        and rank % (8 * n_row) == 0
        and 2 * rank <= min(rows_tile, piece)
        and n_row & (n_row - 1) == 0
        and n_row >= max(8, 2 * n_col)
        and rank % (8 * CHUNKS) == 0
        and n_row > LOADS_AHEAD
        and 6 * rows_tile * cols_tile + 19 * rank * cols_tile <= FULL_VMEM
    )
    if not fits:
        return plain_body(covariance, estimate, dual_var, start_basis)
    return fast_body(n_row, n_col, covariance, estimate, dual_var, start_basis)


def solution(mesh):
    return jax.shard_map(
        body,
        mesh=mesh,
        in_specs=(P("row", "col"), P("row", "col"), P("row", "col"), P("row", None)),
        out_specs=(P("row", "col"), P("row", "col")),
        check_vma=False,
    )
```

```python
import functools

import jax
import jax.numpy as jnp
from jax import lax
from jax.experimental import pallas as pl
from jax.experimental.pallas import tpu as pltpu
from jax.sharding import PartitionSpec as P

NS_ITERS = 12


penalty = 0.01
threshold = 0.2
base_level = 10.0
highest = lax.Precision.HIGHEST


def from_root(value, axis, source):
    kept = jnp.where(lax.axis_index(axis) == source, value, 0).astype(value.dtype)
    return lax.psum(kept, axis)


def inner_product(left_side, right_side):
    return lax.dot_general(
        left_side,
        right_side,
        (((0,), (0,)), ((), ())),
        precision=highest,
        preferred_element_type=jnp.float32,
    )


def normalize(mapped, gram_matrix):
    lower_factor = jnp.linalg.cholesky(gram_matrix)
    identity = jnp.eye(gram_matrix.shape[0], dtype=jnp.float32)
    inverse = lax.linalg.triangular_solve(lower_factor, identity, left_side=True, lower=True)
    return jnp.dot(mapped, inverse.T, precision=highest, preferred_element_type=jnp.float32)


def response_of(ritz_matrix):
    identity = jnp.eye(ritz_matrix.shape[0], dtype=jnp.float32)
    square = (
        jnp.dot(ritz_matrix, ritz_matrix, precision=highest, preferred_element_type=jnp.float32)
        + 4.0 * penalty * identity
    )
    frobenius = jnp.sqrt(jnp.sum(square * square))

    def newton(sweep_index, state_pair):
        iterate, partner = state_pair
        factor = 0.5 * (
            3.0 * identity
            - jnp.dot(partner, iterate, precision=highest, preferred_element_type=jnp.float32)
        )
        return (
            jnp.dot(iterate, factor, precision=highest, preferred_element_type=jnp.float32),
            jnp.dot(factor, partner, precision=highest, preferred_element_type=jnp.float32),
        )

    iterate, partner = lax.fori_loop(0, NS_ITERS, newton, (square / frobenius, identity))
    square_root = jnp.sqrt(frobenius) * iterate
    return (ritz_matrix + square_root) / (2.0 * penalty) - base_level * identity


def column_basis(shifted, row_basis):
    partial_terms = lax.dot_general(
        shifted,
        row_basis,
        (((0,), (0,)), ((), ())),
        precision=highest,
        preferred_element_type=jnp.float32,
    )
    mapped = lax.psum(partial_terms, "row")
    gram_matrix = lax.psum(inner_product(mapped, mapped), "col")
    return normalize(mapped, gram_matrix)


def row_image(shifted, col_basis):
    local_terms = jnp.dot(shifted, col_basis, precision=highest, preferred_element_type=jnp.float32)
    return lax.psum(local_terms, "col")


def row_inner(left_side, right_side):
    return lax.psum(inner_product(left_side, right_side), "row")


def plain_body(covariance, estimate, dual_var, start_basis):
    shifted = penalty * (
        estimate.astype(jnp.float32) - dual_var.astype(jnp.float32)
    ) - covariance.astype(jnp.float32)
    rows_tile = shifted.shape[0]
    cols_tile = shifted.shape[1]
    row_basis = start_basis
    col_basis = column_basis(shifted, row_basis)
    blocks_per_column = lax.axis_size("row") // lax.axis_size("col")
    row_index = lax.axis_index("row")
    own_block = lax.dynamic_slice_in_dim(
        col_basis, row_index % blocks_per_column * rows_tile, rows_tile, 0
    )
    row_basis = from_root(own_block, "col", row_index // blocks_per_column)
    product = row_image(shifted, col_basis)
    raw_ritz = row_inner(row_basis, product)
    ritz_matrix = 0.5 * (raw_ritz + raw_ritz.T)
    response = response_of(ritz_matrix)
    weighted = jnp.dot(row_basis, response, precision=highest, preferred_element_type=jnp.float32)
    theta_tile = lax.dot_general(
        weighted,
        col_basis,
        (((1,), (1,)), ((), ())),
        precision=highest,
        preferred_element_type=jnp.float32,
    )
    row_ids = row_index * rows_tile + lax.broadcasted_iota(jnp.int32, (rows_tile, 1), 0)
    col_ids = lax.axis_index("col") * cols_tile + lax.broadcasted_iota(jnp.int32, (1, cols_tile), 1)
    theta_tile = theta_tile + jnp.where(row_ids == col_ids, base_level, 0.0)
    mixture = theta_tile + dual_var.astype(jnp.float32)
    clipped = jnp.clip(mixture, -threshold, threshold)
    return (mixture - clipped, clipped.astype(jnp.bfloat16))


MESH = pl.DeviceIdType.MESH
VMEM = pl.BlockSpec(memory_space=pltpu.VMEM)
VMEM_BYTES = 40 * 1024 * 1024
FULL_VMEM = 67043328
FRONT_VMEM = 46 * 1024 * 1024 + 512 * 1024
LOADS_AHEAD = 2
CHUNKS = 4
FINISH_ROWS = 256


def high_dot(left_side, right_side, dims):
    return lax.dot_general(
        left_side, right_side, (dims, ((), ())), precision=highest, preferred_element_type=jnp.float32
    )


def split(value):
    upper = value.astype(jnp.bfloat16)
    return upper, (value - upper.astype(jnp.float32)).astype(jnp.bfloat16)


def remote(src, dst, send, recv, target):
    return pltpu.make_async_remote_copy(
        src_ref=src, dst_ref=dst, send_sem=send, recv_sem=recv, device_id=target, device_id_type=MESH
    )


def flip(value, mask, size):
    result, bit = 0, 1
    while bit < size:
        result += (value // bit + mask // bit) % 2 * bit
        bit *= 2
    return result


def front_kernel(
    n_row, n_col, est_hbm, dual_hbm, cov_hbm, basis_hbm, weights_ref, right_hbm, low_hbm, dual_tiles,
    tiles, left_ref, image_ref, away, near, other, zbuf, mc_ref, mr_ref,
    gram, gram_terms, gram_part, gram_planes, gram_sum,
    inner, inner_terms, inner_part, inner_planes, inner_sum,
    inverse_ref, ritz_ref, iterate_ref, partner_ref,
    load_sems, basis_sem, store_sems, *sems
):
    send1, recv1, send2, recv2, send3, recv3, send4, recv4, send5, recv5, send6, recv6 = sems[:12]
    gram_scatter, gram_across, gram_gather, gram_finish, gram_drain = sum_over_mesh(
        n_row, n_col, gram, gram_terms, gram_part, gram_planes, gram_sum, sems[12:18]
    )
    inner_scatter, inner_across, inner_gather, inner_finish, inner_drain = sum_over_mesh(
        n_row, n_col, inner, inner_terms, inner_part, inner_planes, inner_sum, sems[18:24]
    )
    copy = remote
    row, col = lax.axis_index("row"), lax.axis_index("col")
    rank, piece = mc_ref.shape[1:]
    rows_tile = tiles.shape[2]
    chips = n_row // 2
    chip, core = row // 2, row % 2
    sibling = chip * 2 + 1 - core
    ratio = n_row // n_col
    group = n_row // ratio
    cut = rank // CHUNKS
    home = row // ratio

    def works(left, right):
        odd = (left + right) % 2
        return (left == right) | ((odd == 1) & (left < right)) | ((odd == 0) & (left > right))

    working = works(home, col)
    matrices = (est_hbm, dual_hbm, cov_hbm)
    held = (tiles.at[0], dual_tiles, tiles.at[1])

    def load(which, step):
        there = flip(chip, chips - 1 - step // 2, chips)
        where = 2 * there + (1 - core + step) % 2
        columns = pl.ds(pl.multiple_of(where * piece, piece), piece)
        return pltpu.make_async_copy(
            matrices[which].at[:, columns], held[which].at[where], load_sems.at[which, step]
        )

    basis_ref = image_ref.at[:, pl.ds(0, rank)]
    start_basis = pltpu.make_async_copy(basis_hbm, basis_ref, basis_sem)
    start_basis.start()
    for step in range(LOADS_AHEAD):
        for which in range(3):
            load(which, step).start()

    barrier = pltpu.get_barrier_semaphore()

    def greet_row(t, carry):
        pl.semaphore_signal(barrier, inc=1, device_id=((row + t) % n_row, col), device_id_type=MESH)
        return carry

    def greet_col(t, carry):
        pl.semaphore_signal(barrier, inc=1, device_id=(row, (col + t) % n_col), device_id_type=MESH)
        return carry

    lax.fori_loop(1, n_row, greet_row, 0)
    lax.fori_loop(1, n_col, greet_col, 0)

    start_basis.wait()
    depth = min(256, rows_tile)
    for index in range(rows_tile // depth):
        where = slice(index * depth, (index + 1) * depth)
        upper, lower = split(basis_ref[where, :].T)
        left_ref[:rank, where] = upper
        left_ref[rank:, where] = lower
    pl.semaphore_wait(barrier, n_row - 1 + n_col - 1)

    def image_part(step):
        @pl.when(step + LOADS_AHEAD < n_row)
        def _():
            for which in range(3):
                load(which, step + LOADS_AHEAD).start()

        for which in range(3):
            load(which, step).wait()
        where = 2 * flip(chip, chips - 1 - step // 2, chips) + (1 - core + step) % 2

        def product(which):
            return jnp.dot(left_ref[...], held[which][where], preferred_element_type=jnp.float32)

        both = penalty * (product(0) - product(1)) - product(2)
        return both[:rank] + both[rank:]

    def to_sibling(t):
        return copy(away.at[t], near.at[t], send1.at[t], recv1.at[t], (sibling, col))

    def to_chip(t):
        there = flip(chip, chips - 1 - t, chips)
        return copy(near.at[t], other.at[t], send2.at[t], recv2.at[t], (2 * there + core, col))

    def sweep(t, carry):
        away[t] = image_part(2 * t)
        to_sibling(t).start()
        part = image_part(2 * t + 1)
        to_sibling(t).wait_recv()
        near[t] = near[t] + part

        @pl.when(t < chips - 1)
        def _():
            to_chip(t).start()

        return carry

    lax.fori_loop(0, chips, sweep, 0)
    total = near[chips - 1]
    for t in range(chips - 1):
        to_chip(t).wait_recv()
        total += other[t]
    mc_ref[row] = total

    own = mc_ref.at[row]

    def along(source, way, part):
        block = own if source is None else zbuf.at[source]
        source = col if source is None else source
        lines = pl.ds(part * cut, cut)
        return copy(
            block.at[lines], zbuf.at[source, lines],
            send4.at[(way + 1) // 2, source, part], recv4.at[source, part], (row, col + way),
        )

    def start_along(parts):
        for part in parts:
            @pl.when(col + 1 < n_col)
            def _():
                along(None, 1, part).start()

            @pl.when(col >= 1)
            def _():
                along(None, -1, part).start()

    wide = double(own[...], 0)
    wide = lax.dot_general(
        wide, wide, (((1,), (1,)), ((), ())), preferred_element_type=jnp.float32
    )
    wide = wide[:rank] + wide[rank:]
    gram[...] = (wide[:, :rank] + wide[:, rank:]).reshape(gram.shape)
    gram_scatter()
    start_along(range(CHUNKS // 2))

    def plane(t):
        return copy(own, own, send3.at[t], recv3.at[t], (2 * flip(chip, t + 1, chips) + core, col))

    def arrived(t):
        return mc_ref.at[2 * flip(chip, t, chips) + core]

    def pair(t):
        block = arrived(t)
        return copy(block, block, send5.at[t], recv5.at[t], (sibling, col))

    for t in range(chips - 2):
        plane(t).start()
    pair(0).start()

    def onward(source, part):
        target = source * ratio + row // group
        slot = row % group
        lines = pl.ds(part * cut, cut)
        hop = copy(
            zbuf.at[source, lines], mr_ref.at[slot, lines],
            send6.at[source, part], recv6.at[slot, part], (target, col),
        )
        return hop, target

    def send_onward(source, part):
        hop, target = onward(source, part)

        @pl.when(target != row)
        def _():
            hop.start()

        @pl.when(target == row)
        def _():
            lines = slice(part * cut, (part + 1) * cut)
            mr_ref[row % group, lines] = zbuf[source, lines]

    def serve(source, way, part):
        @pl.when((source >= 0) & (source < n_col))
        def _():
            along(source, way, part).wait_recv()

            @pl.when((col + way >= 0) & (col + way < n_col))
            def _():
                along(source, way, part).start()

            @pl.when(works(source, col))
            def _():
                send_onward(source, part)

    def serve_half(hop, half):
        for part in range(CHUNKS // 2):
            for k in range(2):
                @pl.when(half == k)
                def _():
                    serve(col - hop, 1, k * (CHUNKS // 2) + part)
                    serve(col + hop, -1, k * (CHUNKS // 2) + part)

    image_ref[...] = jnp.zeros_like(image_ref)
    strip = min(1024, rows_tile)

    def apply(where):
        upper, lower = split(mc_ref[where].T)
        right = jnp.concatenate([upper, lower], axis=1)

        def one(index, carry):
            rows = pl.ds(pl.multiple_of(index * strip, strip), strip)

            def product(which):
                return jnp.dot(held[which][where, rows, :], right, preferred_element_type=jnp.float32)

            image_ref[rows, :] += penalty * (product(0) - product(1)) - product(2)
            return carry

        lax.fori_loop(0, rows_tile // strip, one, 0)

    def apply_chip(t, swap):
        apply(2 * flip(chip, t, chips) + (core + swap) % 2)

    def wait_pair(t):
        block = mc_ref.at[2 * flip(chip, t, chips) + 1 - core]
        copy(own, block, send5.at[t], recv5.at[t], (sibling, col)).wait_recv()

    def take(t):
        copy(own, arrived(t), send3.at[t - 1], recv3.at[t - 1], (row, col)).wait_recv()
        pair(t).start()

    def stage(j, carry):
        t = j // 2

        @pl.when(j == 2)
        def _():
            gram_gather()
            plane(chips - 2).start()
            for other_chip in range(1, chips - 1):
                take(other_chip)

        @pl.when(j == n_row - 3)
        def _():
            take(chips - 1)

        @pl.when(j % 2 == 1)
        def _():
            wait_pair(t)

        @pl.when(working)
        def _():
            apply_chip(t, j % 2)

        @pl.when(j == 0)
        def _():
            gram_across()
            start_along(range(CHUNKS // 2, CHUNKS))

        @pl.when(t + 1 < n_col)
        def _():
            serve_half(t + 1, j % 2)

        @pl.when(j == 2 * n_col - 3)
        def _():
            for source in range(n_col):
                @pl.when((source != col) & jnp.logical_not(works(source, col)))
                def _():
                    for part in range(CHUNKS):
                        send_onward(source, part)

        return carry

    lax.fori_loop(0, n_row, stage, 0)
    gram_finish()
    third = -(-rank // 24) * 8
    inverse_ref[...] = gram_sum[...].reshape(rank, rank)

    def wait_rows():
        for k in range(group):
            @pl.when((home != col) & ((row % ratio) * group + k != row))
            def _():
                for part in range(CHUNKS):
                    lines = pl.ds(part * cut, cut)
                    copy(
                        zbuf.at[0, lines], mr_ref.at[k, lines],
                        send6.at[0, part], recv6.at[k, part], (sibling, col),
                    ).wait_recv()

    @pl.when(home == col)
    def _():
        for k in range(group):
            mr_ref[k] = mc_ref[(row % ratio) * group + k]

    @pl.when(working)
    def _():
        wait_rows()
        ritz = jnp.zeros((2 * rank, 2 * rank), jnp.float32)
        for k in range(group):
            rows = slice(k * piece, (k + 1) * piece)
            ritz += jnp.dot(
                double(mr_ref[k], 0),
                double(image_ref[rows, :rank] + image_ref[rows, rank:], 1),
                preferred_element_type=jnp.float32,
            )
        ritz = ritz[:rank] + ritz[rank:]
        times = jnp.where(home == col, 1.0, 2.0)
        inner[...] = (times * (ritz[:, :rank] + ritz[:, rank:])).reshape(inner.shape)

    @pl.when(jnp.logical_not(working))
    def _():
        inner[...] = jnp.zeros_like(inner)

    inner_scatter()
    inverse_ref[...] = invert(inverse_ref[...], 0, third)
    inner_across()
    inverse_ref[...] = invert(inverse_ref[...], third, 2 * third)
    inner_gather()
    inverse_ref[...] = invert(inverse_ref[...], 2 * third, rank)

    def prepare(k, carry):
        upper, lower = split(mc_ref[k])
        tiles[0, k, :rank, :] = upper
        tiles[0, k, rank : 2 * rank, :] = upper
        tiles[0, k, 2 * rank : 3 * rank, :] = lower
        return carry

    lax.fori_loop(0, n_row, prepare, 0)
    store_right = pltpu.make_async_copy(
        tiles.at[0, :, pl.ds(0, 2 * rank)], right_hbm, store_sems.at[0]
    )
    store_low = pltpu.make_async_copy(
        tiles.at[0, :, pl.ds(2 * rank, rank)], low_hbm, store_sems.at[1]
    )
    store_right.start()
    store_low.start()
    inner_finish()
    update = response_times_inverse(
        inner_sum[...].reshape(rank, rank), inverse_ref, ritz_ref, iterate_ref, partner_ref
    )
    partner_ref[...] = update

    @pl.when(jnp.logical_not(working))
    def _():
        wait_rows()

    for k in range(group):
        weights_ref[k * piece : (k + 1) * piece, :] = double(
            fine_dot(mr_ref[k].T, partner_ref[...]), 1
        )
    gram_drain()
    inner_drain()
    store_right.wait()
    store_low.wait()
    for t in range(chips):
        to_sibling(t).wait_send()
        pair(t).wait_send()
    for t in range(chips - 1):
        to_chip(t).wait_send()
        plane(t).wait_send()

    for part in range(CHUNKS):
        @pl.when(col + 1 < n_col)
        def _():
            along(None, 1, part).wait_send()

        @pl.when(col >= 1)
        def _():
            along(None, -1, part).wait_send()

        for s in range(1, n_col):
            for source, way in ((col - s, 1), (col + s, -1)):
                @pl.when((source >= 0) & (source < n_col))
                def _():
                    @pl.when((col + way >= 0) & (col + way < n_col))
                    def _():
                        along(source, way, part).wait_send()

                    hop, target = onward(source, part)

                    @pl.when(target != row)
                    def _():
                        hop.wait_send()


def front(matrices, start_basis, n_row, n_col):
    rows_tile, cols_tile = matrices[0].shape
    rank = start_basis.shape[1]
    piece = cols_tile // n_row
    chips, ratio = n_row // 2, n_row // n_col
    group = n_row // ratio
    dma = pltpu.SemaphoreType.DMA
    block = (rank // n_row, rank)
    sum_buffers = [
        pltpu.VMEM((n_row, *block), jnp.float32),
        pltpu.VMEM((n_row, *block), jnp.float32),
        pltpu.VMEM(block, jnp.float32),
        pltpu.VMEM((n_col, *block), jnp.float32),
        pltpu.VMEM((n_row, *block), jnp.float32),
    ]
    sum_sems = [dma((n_row,))] * 2 + [dma((n_col,))] * 2 + [dma((n_row,))] * 2
    return pl.pallas_call(
        functools.partial(front_kernel, n_row, n_col),
        in_specs=[pl.BlockSpec(memory_space=pl.ANY)] * 4,
        out_specs=[VMEM] + [pl.BlockSpec(memory_space=pl.ANY)] * 2 + [VMEM],
        out_shape=(
            pltpu.VMEM((rows_tile, 2 * rank), jnp.bfloat16),
            jax.ShapeDtypeStruct((n_row, 2 * rank, piece), jnp.bfloat16),
            jax.ShapeDtypeStruct((n_row, rank, piece), jnp.bfloat16),
            pltpu.VMEM((n_row, rows_tile, piece), jnp.bfloat16),
        ),
        scratch_shapes=[
            pltpu.VMEM((2, n_row, rows_tile, piece), jnp.bfloat16),
            pltpu.VMEM((2 * rank, rows_tile), jnp.bfloat16),
            pltpu.VMEM((rows_tile, 2 * rank), jnp.float32),
            pltpu.VMEM((chips, rank, piece), jnp.float32),
            pltpu.VMEM((chips, rank, piece), jnp.float32),
            pltpu.VMEM((chips - 1, rank, piece), jnp.float32),
            pltpu.VMEM((n_col, rank, piece), jnp.float32),
            pltpu.VMEM((n_row, rank, piece), jnp.float32),
            pltpu.VMEM((group, rank, piece), jnp.float32),
            *sum_buffers, *sum_buffers,
            *[pltpu.VMEM((rank, rank), jnp.float32)] * 4,
            dma((3, n_row)), dma, dma((2,)),
            dma((chips,)), dma((chips,)),
            dma((chips - 1,)), dma((chips - 1,)),
            dma((chips - 1,)), dma((chips - 1,)),
            dma((2, n_col, CHUNKS)), dma((n_col, CHUNKS)),
            dma((chips,)), dma((chips,)),
            dma((n_col, CHUNKS)), dma((group, CHUNKS)),
            *sum_sems, *sum_sems,
        ],
        compiler_params=pltpu.CompilerParams(
            collective_id=0, has_side_effects=True, vmem_limit_bytes=FRONT_VMEM
        ),
    )(*matrices, start_basis)


def sum_over_mesh(n_row, n_col, term, terms, part, planes, out, sems):
    send1, recv1, send2, recv2, send3, recv3 = sems
    row, col = lax.axis_index("row"), lax.axis_index("col")

    def first(t):
        there = (row + t) % n_row
        return remote(term.at[there], terms.at[t], send1.at[t], recv1.at[t], (there, col))

    def second(t):
        there = (col + t) % n_col
        return remote(part, planes.at[col], send2.at[t], recv2.at[col], (row, there))

    def third(t):
        there = (row + t) % n_row
        return remote(out.at[row], out.at[row], send3.at[t], recv3.at[t], (there, col))

    def scatter():
        for t in range(1, n_row):
            first(t).start()

    def across():
        summed = term[row]
        for t in range(1, n_row):
            first(t).wait_recv()
            summed += terms[t]
        part[...] = summed
        for t in range(1, n_col):
            second(t).start()
        planes[col] = summed

    def gather():
        for t in range(1, n_col):
            source = (col + t) % n_col
            remote(part, planes.at[source], send2.at[t], recv2.at[source], (row, source)).wait_recv()
        out[row] = jnp.sum(planes[...], axis=0)
        for t in range(1, n_row):
            third(t).start()

    def finish():
        for t in range(1, n_row):
            source = (row + n_row - t) % n_row
            remote(out.at[row], out.at[source], send3.at[t], recv3.at[t], (source, col)).wait_recv()

    def drain():
        for t in range(1, n_row):
            first(t).wait_send()
            third(t).wait_send()
        for t in range(1, n_col):
            second(t).wait_send()

    return scatter, across, gather, finish, drain


def invert(value, first, last):
    rank = value.shape[0]
    row_ids = lax.broadcasted_iota(jnp.int32, (rank, rank), 0)
    col_ids = lax.broadcasted_iota(jnp.int32, (rank, rank), 1)
    line_ids = lax.broadcasted_iota(jnp.int32, (1, rank), 1)
    for k in range(first, last):
        pivot = 1.0 / value[k : k + 1, k : k + 1]
        column = value[:, k : k + 1]
        line = jnp.where(line_ids == k, 1.0, value[k : k + 1, :]) * pivot
        value = jnp.where(
            row_ids == k, line, jnp.where(col_ids == k, 0.0, value) - column * line
        )
    return value


def double(value, axis):
    return jnp.concatenate(split(value), axis=axis)


def fine_dot(left_side, right_side):
    right = double(right_side, 1)
    both = jnp.dot(
        double(left_side, 1),
        jnp.concatenate([right, right], axis=0),
        preferred_element_type=jnp.float32,
    )
    width = right_side.shape[1]
    return both[:, :width] + both[:, width:]


def response_times_inverse(raw, inverse_ref, ritz_ref, iterate_ref, partner_ref):
    rank = raw.shape[0]
    row_ids = lax.broadcasted_iota(jnp.int32, (rank, rank), 0)
    col_ids = lax.broadcasted_iota(jnp.int32, (rank, rank), 1)
    identity = jnp.where(row_ids == col_ids, 1.0, 0.0)
    ritz_ref[...] = fine_dot(inverse_ref[...], 0.5 * (raw + raw.T))
    square = fine_dot(ritz_ref[...], ritz_ref[...]) + 4.0 * penalty * identity
    frobenius = jnp.sqrt(jnp.sum(square * square.T, keepdims=True))
    start = square / frobenius
    factor = 1.5 * identity - 0.5 * start
    iterate_ref[...] = fine_dot(start, factor)
    partner_ref[...] = factor

    def newton(step, carry):
        iterate, partner = iterate_ref[...], partner_ref[...]
        factor = 1.5 * identity - 0.5 * fine_dot(partner, iterate)
        iterate_ref[...] = fine_dot(iterate, factor)
        partner_ref[...] = fine_dot(factor, partner)
        return carry

    lax.fori_loop(1, NS_ITERS, newton, 0)
    root = jnp.sqrt(frobenius) * iterate_ref[...]
    response = (ritz_ref[...] + root) / (2.0 * penalty) - base_level * identity
    return fine_dot(response, inverse_ref[...])


def finish_kernel(weights_ref, right_ref, low_ref, dual_ref, est_ref, clip_ref):
    step = pl.program_id(0)
    count, rank, piece = low_ref.shape
    depth = est_ref.shape[0]
    lines = pl.ds(pl.multiple_of(step * depth, depth), depth)
    n_grid = pl.num_programs(0)
    row_start = (lax.axis_index("row") * n_grid + step) * depth
    gap = (
        lax.broadcasted_iota(jnp.int32, (depth, piece), 1)
        - lax.broadcasted_iota(jnp.int32, (depth, piece), 0)
    )
    for k in range(count):
        where = slice(k * piece, (k + 1) * piece)
        col_start = lax.axis_index("col") * (count * piece) + k * piece
        theta = jnp.dot(weights_ref[lines, :], right_ref[k], preferred_element_type=jnp.float32)
        theta += jnp.dot(weights_ref[lines, :rank], low_ref[k], preferred_element_type=jnp.float32)
        theta += jnp.where(gap == row_start - col_start, base_level, 0.0)
        mixture = theta + dual_ref[k, lines, :].astype(jnp.float32)
        clipped = jnp.clip(mixture, -threshold, threshold)
        est_ref[:, where] = mixture - clipped
        clip_ref[:, where] = clipped.astype(jnp.bfloat16)


def near_by(value):
    return pltpu.with_memory_space_constraint(value, pltpu.VMEM)


def finish(weights, right, low, dual_tiles):
    count, rows_tile, piece = dual_tiles.shape
    whole = (rows_tile, count * piece)
    cols_tile = whole[1]
    depth = min(FINISH_ROWS, rows_tile)
    wide = pl.BlockSpec((depth, cols_tile), lambda step: (step, 0))
    return pl.pallas_call(
        finish_kernel,
        grid=(rows_tile // depth,),
        in_specs=[
            VMEM,
            pl.BlockSpec(right.shape, lambda step: (0, 0, 0)),
            pl.BlockSpec(low.shape, lambda step: (0, 0, 0)),
            VMEM,
        ],
        out_specs=(wide, wide),
        out_shape=(
            jax.ShapeDtypeStruct(whole, jnp.float32),
            jax.ShapeDtypeStruct(whole, jnp.bfloat16),
        ),
        compiler_params=pltpu.CompilerParams(
            dimension_semantics=("arbitrary",), vmem_limit_bytes=VMEM_BYTES
        ),
    )(near_by(weights), right, low, near_by(dual_tiles))


def fast_body(n_row, n_col, covariance, estimate, dual_var, start_basis):
    rows_tile, cols_tile = covariance.shape
    rank = start_basis.shape[1]
    matrices = (estimate, dual_var, covariance)
    return finish(*front(matrices, start_basis, n_row, n_col))


def body(covariance, estimate, dual_var, start_basis):
    n_row, n_col = lax.axis_size("row"), lax.axis_size("col")
    rows_tile, cols_tile = covariance.shape
    rank = start_basis.shape[1]
    piece = cols_tile // n_row
    fits = (
        n_row % 2 == 0
        and n_row % n_col == 0
        and cols_tile % n_row == 0
        and piece % 128 == 0
        and rows_tile % piece == 0
        and rank % 128 == 0
        and rank % (8 * n_row) == 0
        and 3 * rank <= min(rows_tile, piece)
        and n_row & (n_row - 1) == 0
        and n_row >= max(8, 2 * n_col)
        and rank % (8 * CHUNKS) == 0
        and n_row > LOADS_AHEAD
        and 6 * rows_tile * cols_tile + 23 * rank * cols_tile <= FULL_VMEM
    )
    if not fits:
        return plain_body(covariance, estimate, dual_var, start_basis)
    return fast_body(n_row, n_col, covariance, estimate, dual_var, start_basis)


def solution(mesh):
    return jax.shard_map(
        body,
        mesh=mesh,
        in_specs=(P("row", "col"), P("row", "col"), P("row", "col"), P("row", None)),
        out_specs=(P("row", "col"), P("row", "col")),
        check_vma=False,
    )
```
